32 devices in a mesh: section: 4 (over z), tp: 2 (over y), dp: 4 (over x, core).
Axes of the slice: x: 2, y: 2, z: 4, core: 2. Of those that a mesh axis runs over, the one named last changes fastest.
Arguments:
- incoming: bfloat16 [4, 8, 128, 2304], P('section', ('dp', 'tp')), parts along dimension 1, may hold values from -6 to 6
- fresh_rows: bfloat16 [6, 8, 128, 2304], P(None, ('dp', 'tp')), parts along dimension 1, may hold values from -6 to 6
- entry_order: int32 [24], P('dp'), parts along dimension 0, may hold values from 0 to 5, each once
- flight_lengths: int32 [4, 8], P('section', 'dp'), parts along dimension 1, may hold values from 16 to 128
- pre_gain: float32 [4, 2304], P('section'), may hold values from 0.1 to 1.9
- post_gain: float32 [4, 2304], P('section'), may hold values from 0.1 to 1.9
- w_query: bfloat16 [4, 2304, 2048], P('section', None, 'tp'), may hold values from -0.125 to 0.125
- key_weight: bfloat16 [4, 2304, 1024], P('section', None, 'tp'), may hold values from -0.125 to 0.125
- value_weight: bfloat16 [4, 2304, 1024], P('section', None, 'tp'), may hold values from -0.125 to 0.125
- w_out: bfloat16 [4, 2048, 2304], P('section', 'tp'), may hold values from -0.125 to 0.125
Outputs:
- produced: bfloat16 [4, 8, 128, 2304], P('section', ('dp', 'tp')), parts along dimension 1
- advanced: bfloat16 [4, 8, 128, 2304], P('section', ('dp', 'tp')), parts along dimension 1
The draws below stay inside these ranges and needn't reach their ends.
There are 4 independent parts, one for each index of `dp`. The reference program is written for one: setup_inputs(seed, part) draws one part's arguments, and reference() takes and returns one part's arrays. A program takes and returns all parts, laid end to end along the dimension named above; an argument that names none is the same for every part. Nothing has to cross between parts.
Inputs may be any that keep to these rules, and one draw needn't show every extreme that they name: `entry_order`: each waiting microbatch appears once.
All inputs are finite; a program needn't handle non-finite values.
Results may differ from the reference program's by a relative error of at most 0.012.
Values may be sent and summed in bfloat16 or wider, within the bound.
No kernel may reach another device: no remote copies, remote signals or barrier semaphores. Data moves between devices by JAX's collectives and lax.ppermute only.
A program may use at most 64 MiB of HBM per device.

```python
import jax
import jax.numpy as jnp
from jax import lax

MODEL_WIDTH = 2304
QUERY_HEADS = 16
KEY_VALUE_HEADS = 8
HEAD_WIDTH = 128
SEQUENCE_TOKENS = 128
POOL = 6
MICRO_SEQUENCES = 2
N_SECTION = 4
N_TP = 2


def set_ends(result, rng, least, top_value):
    place = [jax.random.randint(jax.random.fold_in(rng, axis), (), 0, length) for axis, length in enumerate(result.shape)]
    main_axis = result.shape.index(max(result.shape))
    beside = place[:main_axis] + [(place[main_axis] + 1) % result.shape[main_axis]] + place[main_axis + 1:]
    return result.at[tuple(place)].set(least).at[tuple(beside)].set(top_value)


def shard_levels(stream_key, extent, cuts, smallest, largest):
    level = 1.0
    for axis_at, blocks in cuts:
        heights = jax.random.uniform(jax.random.fold_in(jax.random.fold_in(stream_key, 6), axis_at), (blocks,), jnp.float32, smallest / len(cuts), largest / len(cuts))
        level = level * jnp.repeat(jnp.exp(heights), extent[axis_at] // blocks).reshape((-1,) + (1,) * (len(extent) - 1 - axis_at))
    return level


def normal_values(rng, shape, scale, bound, pieces=(), kind=jnp.bfloat16):
    factor_of = shard_levels(rng, shape, pieces, -0.22, 0.18) if pieces else 1.0
    values = jax.random.normal(rng, shape, jnp.float32) * scale * factor_of
    return jnp.minimum(jnp.maximum(values, -bound), bound).astype(kind)


def setup_inputs(seed: int = 0, part: int = 0) -> dict:
    splits = jax.random.split(jax.random.key(seed), 11)
    part_keys = jax.random.split(jax.random.fold_in(splits[10], part), 11)
    return {
        "incoming": normal_values(part_keys[0], (N_SECTION, MICRO_SEQUENCES, SEQUENCE_TOKENS, MODEL_WIDTH), 1.0, 6.0, ((0, 4), (1, 2))),
        "fresh_rows": normal_values(part_keys[1], (POOL, MICRO_SEQUENCES, SEQUENCE_TOKENS, MODEL_WIDTH), 1.0, 6.0, ((1, 2),)),
        "entry_order": jax.random.permutation(part_keys[2], POOL).astype(jnp.int32),
        "flight_lengths": set_ends(jax.random.randint(part_keys[3], (N_SECTION, MICRO_SEQUENCES), SEQUENCE_TOKENS // 8, SEQUENCE_TOKENS + 1), jax.random.fold_in(part_keys[3], 1), SEQUENCE_TOKENS // 8, SEQUENCE_TOKENS).astype(jnp.int32),
        "pre_gain": jnp.clip(1.0 + 0.18 * jax.random.normal(splits[4], (N_SECTION, MODEL_WIDTH), jnp.float32), 0.1, 1.9),
        "post_gain": jnp.clip(1.0 + 0.18 * jax.random.normal(splits[5], (N_SECTION, MODEL_WIDTH), jnp.float32), 0.1, 1.9),
        "w_query": normal_values(splits[6], (N_SECTION, MODEL_WIDTH, QUERY_HEADS * HEAD_WIDTH), MODEL_WIDTH ** -0.5, 0.125, ((0, 4), (2, 2))),
        "key_weight": normal_values(splits[7], (N_SECTION, MODEL_WIDTH, KEY_VALUE_HEADS * HEAD_WIDTH), MODEL_WIDTH ** -0.5, 0.125, ((0, 4), (2, 2))),
        "value_weight": normal_values(splits[8], (N_SECTION, MODEL_WIDTH, KEY_VALUE_HEADS * HEAD_WIDTH), MODEL_WIDTH ** -0.5, 0.125, ((0, 4), (2, 2))),
        "w_out": normal_values(splits[9], (N_SECTION, QUERY_HEADS * HEAD_WIDTH, MODEL_WIDTH), (QUERY_HEADS * HEAD_WIDTH) ** -0.5, 0.125, ((0, 4), (1, 2))),
    }


EPSILON = 1e-06
SOFT_CAP = 50.0
QUERY_SCALE = 144.0 ** (-0.5)

def normalize(values, gain):
    return values * lax.rsqrt(lax.optimization_barrier(jnp.mean(values * values, -1, keepdims=True)) + EPSILON) * gain

def apply_rotary(values, token_positions):
    half = values.shape[-1] // 2
    freq = 10000.0 ** (-2.0 * jnp.arange(half).astype(jnp.float32) / values.shape[-1])
    angle = token_positions[:, None].astype(jnp.float32) * freq[None, :]
    cosine = jnp.cos(angle)[:, None, :]
    sine = jnp.sin(angle)[:, None, :]
    first = values[..., :half]
    second = values[..., half:]
    return jnp.concatenate([first * cosine - second * sine, second * cosine + first * sine], -1)

def layer(held, lengths, gain_before, gain_after, w_query, key_weight, value_weight, w_out):
    widened = held.astype(jnp.float32).reshape(MICRO_SEQUENCES * SEQUENCE_TOKENS, MODEL_WIDTH)
    normalized_input = normalize(widened, gain_before).astype(jnp.bfloat16)
    token_positions = jnp.tile(jnp.arange(SEQUENCE_TOKENS).astype(jnp.int32), MICRO_SEQUENCES)
    query_matrix = jnp.dot(normalized_input, w_query, preferred_element_type=jnp.float32).reshape(MICRO_SEQUENCES * SEQUENCE_TOKENS, QUERY_HEADS, HEAD_WIDTH)
    query_matrix = apply_rotary(query_matrix, token_positions).astype(jnp.bfloat16).reshape(MICRO_SEQUENCES, SEQUENCE_TOKENS, KEY_VALUE_HEADS, QUERY_HEADS // KEY_VALUE_HEADS, HEAD_WIDTH)
    projected_keys = apply_rotary(jnp.dot(normalized_input, key_weight, preferred_element_type=jnp.float32).reshape(MICRO_SEQUENCES * SEQUENCE_TOKENS, KEY_VALUE_HEADS, HEAD_WIDTH), token_positions).astype(jnp.bfloat16).reshape(MICRO_SEQUENCES, SEQUENCE_TOKENS, KEY_VALUE_HEADS, HEAD_WIDTH)
    projected_values = jnp.dot(normalized_input, value_weight, preferred_element_type=jnp.float32).astype(jnp.bfloat16).reshape(MICRO_SEQUENCES, SEQUENCE_TOKENS, KEY_VALUE_HEADS, HEAD_WIDTH)
    scores = jnp.einsum('bqkgd,bskd->bkgqs', query_matrix.astype(jnp.float32), projected_keys.astype(jnp.float32)) * QUERY_SCALE
    capped = SOFT_CAP * jnp.tanh(scores / SOFT_CAP)
    position = jnp.arange(SEQUENCE_TOKENS).astype(jnp.int32)
    causal = position[None, :] <= position[:, None]
    allowed = causal[None, :, :] & (position[None, None, :] < lengths[:, None, None])
    raised = jnp.where(allowed[:, None, None, :, :], jnp.exp(capped), jnp.float32(0.0))
    probs = (raised / lax.optimization_barrier(jnp.sum(raised, -1, keepdims=True))).astype(jnp.bfloat16)
    mixed = jnp.einsum('bkgqs,bskd->bqkgd', probs.astype(jnp.float32), projected_values.astype(jnp.float32)).astype(jnp.bfloat16)
    mixed = mixed.reshape(MICRO_SEQUENCES * SEQUENCE_TOKENS, N_TP, QUERY_HEADS * HEAD_WIDTH // N_TP)
    grouped = jnp.einsum('sjc,jcd->jsd', mixed.astype(jnp.float32), w_out.reshape(N_TP, QUERY_HEADS * HEAD_WIDTH // N_TP, MODEL_WIDTH).astype(jnp.float32))
    grouped = lax.optimization_barrier(grouped.astype(jnp.bfloat16))
    branch_sum = lax.optimization_barrier(jnp.sum(grouped.astype(jnp.float32), 0))
    return (widened + normalize(branch_sum, gain_after)).astype(jnp.bfloat16).reshape(MICRO_SEQUENCES, SEQUENCE_TOKENS, MODEL_WIDTH)

def reference(incoming, fresh_rows, entry_order, flight_lengths, pre_gain, post_gain, w_query, key_weight, value_weight, w_out):

    def section_step(section):
        return layer(incoming[section], flight_lengths[section], pre_gain[section], post_gain[section], w_query[section], key_weight[section], value_weight[section], w_out[section])
    produced = lax.map(section_step, jnp.arange(N_SECTION).astype(jnp.int32))
    chosen = entry_order[0]
    advanced = jnp.concatenate([fresh_rows[chosen][None], produced[:-1]], 0)
    return (produced, advanced)
```

```python
import functools

import jax
import jax.numpy as jnp
import numpy as np
from jax import lax
from jax.experimental import pallas as pl
from jax.experimental.pallas import tpu as pltpu
from jax.sharding import PartitionSpec as P

HEAD_WIDTH = 128
EPSILON = 1e-06
SOFT_CAP = 50.0
QUERY_SCALE = 144.0 ** (-0.5)

VMEM = pl.BlockSpec(memory_space=pltpu.VMEM)
SMEM = pl.BlockSpec(memory_space=pltpu.SMEM)
HBM = pl.BlockSpec(memory_space=pl.ANY)
F32 = jnp.float32
BF16 = jnp.bfloat16


def vmem_out(shape, dtype=BF16):
    return pltpu.VMEM(shape, dtype)


def pieces_of(seq_len):
    half, quarter = seq_len // 2, seq_len // 4
    return (
        (0, half, ((0, half),)),
        (half, seq_len, ((half, half + quarter), (half + quarter, seq_len))),
    )


def rotary_tables(seq_len):
    half = HEAD_WIDTH // 2
    freq = np.float32(10000.0) ** (np.float32(-2.0) * np.arange(half, dtype=np.float32) / np.float32(HEAD_WIDTH))
    angle = np.arange(seq_len, dtype=np.float32)[:, None] * freq[None, :]
    cosine, sine = np.cos(angle), np.sin(angle)
    return (
        np.concatenate([cosine, cosine], 1).astype(np.float32),
        np.concatenate([-sine, sine], 1).astype(np.float32),
    )


def rotate(values, cosine, sine):
    return values * cosine + pltpu.roll(values, HEAD_WIDTH // 2, 1) * sine


def attend(normed, first, length, cosine, sine, prev, wq, wk, wv, wo, ready, sinks, kv_sinks):
    rows = normed.shape[0]
    kv_cols = wk.shape[1]
    heads_kv = kv_cols // HEAD_WIDTH
    group = wq.shape[1] // kv_cols
    total = first + rows
    dot = functools.partial(jnp.dot, preferred_element_type=F32)
    ready("k")
    keys = dot(normed, wk[...])
    ready("v")
    vals = dot(normed, wv[...]).astype(BF16)
    keys = [
        rotate(keys[:, g * HEAD_WIDTH : (g + 1) * HEAD_WIDTH], cosine, sine).astype(BF16)
        for g in range(heads_kv)
    ]
    if kv_sinks is not None:
        for g in range(heads_kv):
            kv_sinks[0][:, g * HEAD_WIDTH : (g + 1) * HEAD_WIDTH] = keys[g]
        kv_sinks[1][...] = vals
    q_pos = lax.broadcasted_iota(jnp.int32, (rows, total), 0) + first
    k_pos = lax.broadcasted_iota(jnp.int32, (rows, total), 1)
    allowed = (k_pos <= q_pos) & (k_pos < length)
    allowed = jnp.concatenate([allowed] * group, 0)
    mixed = []
    for g in range(heads_kv):
        ready("q", g)
        width = group * HEAD_WIDTH
        q = dot(normed, wq[:, g * width : (g + 1) * width])
        q = jnp.concatenate(
            [rotate(q[:, j * HEAD_WIDTH : (j + 1) * HEAD_WIDTH], cosine, sine) for j in range(group)], 0
        ).astype(BF16)
        kg, vg = keys[g], vals[:, g * HEAD_WIDTH : (g + 1) * HEAD_WIDTH]
        if prev is not None:
            cols = slice(g * HEAD_WIDTH, (g + 1) * HEAD_WIDTH)
            kg = jnp.concatenate([prev[0][:, cols], kg], 0)
            vg = jnp.concatenate([prev[1][:, cols], vg], 0)
        scores = lax.dot_general(q, kg, (((1,), (1,)), ((), ())), preferred_element_type=F32)
        capped = SOFT_CAP * jnp.tanh(scores * (QUERY_SCALE / SOFT_CAP))
        raised = jnp.where(allowed, jnp.exp(capped), 0.0)
        probs = (raised / jnp.sum(raised, -1, keepdims=True)).astype(BF16)
        out = dot(probs, vg).astype(BF16)
        mixed += [out[j * rows : (j + 1) * rows] for j in range(group)]
    mixed = jnp.concatenate(mixed, 1)
    width = wo.shape[1]
    step = next(s for s in (768, 512, 384, 256, 128, width) if width % s == 0)
    for n, c in enumerate(range(0, width, step)):
        ready("o", n)
        part = dot(mixed, wo[:, c : c + step]).astype(BF16)
        for (a, b), sink in sinks:
            sink[:, c : c + step] = part[a - first : b - first]


def normalize(values, gain):
    return values * lax.rsqrt(jnp.mean(values * values, -1, keepdims=True) + EPSILON) * gain


def own_kernel(axis, spans, nx, n_out, *refs):
    xs, refs = refs[:nx], refs[nx:]
    gain, cosine, sine, lengths, hq, hk, hv, ho = refs[:8]
    outs = refs[8 : 8 + n_out]
    wq, wk, wv, wo = refs[8 + n_out : 12 + n_out]
    sems = refs[12 + n_out]
    kv_cols = wk.shape[1]
    width = wq.shape[1] // (kv_cols // HEAD_WIDTH)
    model = wo.shape[1]
    step = next(s for s in (768, 512, 384, 256, 128, model) if model % s == 0)
    copies = {("k",): (hk, wk, 0, kv_cols), ("v",): (hv, wv, 0, kv_cols)}
    for g in range(kv_cols // HEAD_WIDTH):
        copies["q", g] = (hq, wq, g * width, width)
    for n in range(model // step):
        copies["o", n] = (ho, wo, n * step, step)
    started = {}
    for i, (name, (src, dst, c, w)) in enumerate(copies.items()):
        started[name] = pltpu.make_async_copy(src.at[:, c : c + w], dst.at[:, c : c + w], sems.at[i])
        started[name].start()
    me = lax.axis_index(axis)
    normed = jnp.concatenate([normalize(x[...].astype(F32), gain[...]).astype(BF16) for x in xs], 0)
    attend(
        normed, 0, lengths[0, me], cosine[...], sine[...], None, wq, wk, wv, wo,
        lambda *name: started[name].wait(), list(zip(spans, outs)), None,
    )


def peer_kernel(axis, distance, first, spans, keep, *refs):
    x, gain, cosine, sine, lengths, wq, wk, wv, wo = refs[:9]
    refs = refs[9:]
    prev = None
    if first:
        prev, refs = (refs[0], refs[1]), refs[2:]
    outs, refs = refs[: len(spans)], refs[len(spans) :]
    n = lengths.shape[1]
    owner = lax.rem(lax.axis_index(axis) + (n - distance), n)
    normed = normalize(x[...].astype(F32), gain[...]).astype(BF16)
    rows = x.shape[0]
    attend(
        normed, first, lengths[0, owner], cosine[first : first + rows, :], sine[first : first + rows, :],
        prev, wq, wk, wv, wo, lambda *name: None, list(zip(spans, outs)), refs[:2] if keep else None,
    )


def finish_kernel(offset, *refs):
    own, x, gain = refs[:3]
    others, out = refs[3:-1], refs[-1]
    rows = own.shape[0]
    branch = own[...].astype(F32)
    for other in others:
        branch = branch + other[...].astype(F32)
    held = x[offset : offset + rows, :].astype(F32)
    out[...] = (held + normalize(branch, gain[...])).astype(BF16)


def store_kernel(spans, *refs):
    pieces, out, sems = refs[: len(spans)], refs[-2], refs[-1]
    copies = [
        pltpu.make_async_copy(p, out.at[0, 0, a:b], sems.at[i])
        for i, (p, (a, b)) in enumerate(zip(pieces, spans))
    ]
    for c in copies:
        c.start()
    for c in copies:
        c.wait()


def advance_kernel(axis, spans, *refs):
    pieces, fresh, out, sems = refs[: len(spans)], refs[-3], refs[-2], refs[-1]
    first = lax.axis_index(axis) == 0

    @pl.when(first)
    def _():
        copy = pltpu.make_async_copy(fresh, out.at[0, 0], sems.at[0])
        copy.start()
        copy.wait()

    @pl.when(jnp.logical_not(first))
    def _():
        store_kernel(spans, *pieces, out, sems)


def fresh_kernel(order, fresh_rows, out, sem):
    copy = pltpu.make_async_copy(fresh_rows.at[order[0], 0], out, sem)
    copy.start()
    copy.wait()


def split_kernel(spans, x, *refs):
    outs, sems = refs[:-1], refs[-1]
    copies = [
        pltpu.make_async_copy(x.at[0, 0, a:b], out, sems.at[i])
        for i, (out, (a, b)) in enumerate(zip(outs, spans))
    ]
    for c in copies:
        c.start()
    for c in copies:
        c.wait()


def call(kernel, name, out_shape, in_specs, out_specs, args, scratch=(), us=1.0, limit=16 << 20):
    return pl.pallas_call(
        kernel,
        out_shape=out_shape,
        in_specs=in_specs,
        out_specs=out_specs,
        scratch_shapes=list(scratch),
        name=name,
        cost_estimate=pl.CostEstimate(flops=int(us * 1e7), bytes_accessed=1024, transcendentals=0),
        compiler_params=pltpu.CompilerParams(vmem_limit_bytes=limit),
    )(*args)


def shards(
    incoming,
    fresh_rows,
    entry_order,
    flight_lengths,
    pre_gain,
    post_gain,
    w_query,
    key_weight,
    value_weight,
    w_out,
):
    seq_len, model = incoming.shape[2:]
    chunks = pieces_of(seq_len)
    spans = [span for _, _, inner in chunks for span in inner]
    n_tp = lax.axis_size("tp")
    n_section = lax.axis_size("section")
    wq, wk, wv, wo = w_query[0], key_weight[0], value_weight[0], w_out[0]
    kv_cols = wk.shape[1]
    cosine, sine = (jnp.asarray(t) for t in rotary_tables(seq_len))
    dma = pltpu.SemaphoreType.DMA

    xs = call(
        functools.partial(split_kernel, [(a, b) for a, b, _ in chunks]), "split",
        [vmem_out((b - a, model)) for a, b, _ in chunks], [HBM], [VMEM] * len(chunks),
        [incoming], [dma((len(chunks),))],
    )
    out_of = {d: [(i, (i + d) % n_tp) for i in range(n_tp)] for d in range(n_tp)}
    arrived = {d: [lax.ppermute(x, "tp", out_of[d]) for x in xs] for d in range(1, n_tp)}

    n_copies = 2 + kv_cols // HEAD_WIDTH + model // 128
    own = call(
        functools.partial(own_kernel, "tp", spans, len(xs), len(spans)), "own",
        [vmem_out((b - a, model)) for a, b in spans] + [vmem_out(w.shape) for w in (wq, wk, wv, wo)],
        [VMEM] * len(xs) + [VMEM, VMEM, VMEM, SMEM] + [HBM] * 4, [VMEM] * (len(spans) + 4),
        [*xs, pre_gain, cosine, sine, flight_lengths, wq, wk, wv, wo], [dma((n_copies,))], us=6.0,
    )
    own, weights = own[: len(spans)], own[len(spans) :]
    fresh = call(
        fresh_kernel, "fresh", vmem_out((seq_len, model)), [SMEM, HBM], VMEM,
        [entry_order, fresh_rows], [dma],
    )

    back = {span: [] for span in spans}
    for d in range(1, n_tp):
        kept = []
        for c, (first, last, inner) in enumerate(chunks):
            keep = c + 1 < len(chunks)
            shapes = [vmem_out((b - a, model)) for a, b in inner]
            shapes += [vmem_out((last - first, kv_cols))] * 2 if keep else []
            prev = []
            if first:
                prev = [jnp.concatenate([k[i] for k in kept], 0) if len(kept) > 1 else kept[0][i] for i in range(2)]
            done = call(
                functools.partial(peer_kernel, "tp", d, first, inner, keep), f"peer{c}",
                shapes, [VMEM] * 4 + [SMEM] + [VMEM] * (4 + len(prev)), [VMEM] * len(shapes),
                [arrived[d][c], pre_gain, cosine, sine, flight_lengths, *weights, *prev], us=5.0,
            )
            kept.append(done[len(inner) :])
            for span, part in zip(inner, done):
                back[span].append(lax.ppermute(part, "tp", [(t, s) for s, t in out_of[d]]))

    produced, moved = [], []
    line = [(i, i + 1) for i in range(n_section - 1)]
    for c, (first, last, inner) in enumerate(chunks):
        for span in inner:
            i = spans.index(span)
            piece = call(
                functools.partial(finish_kernel, span[0] - first), "finish",
                vmem_out((span[1] - span[0], model)), [VMEM] * (3 + len(back[span])), VMEM,
                [own[i], xs[c], post_gain, *back[span]], us=1.0,
            )
            produced.append(piece)
            moved.append(lax.ppermute(piece, "section", line))
    full = jax.ShapeDtypeStruct(incoming.shape, incoming.dtype)
    stored = call(
        functools.partial(store_kernel, spans), "store", full, [VMEM] * len(spans), HBM,
        produced, [dma((len(spans),))],
    )
    advanced = call(
        functools.partial(advance_kernel, "section", spans), "advance", full,
        [VMEM] * (len(spans) + 1), HBM, [*moved, fresh], [dma((len(spans),))],
    )
    return stored, advanced


def solution(mesh):
    in_specs = (
        P("section", ("dp", "tp"), None, None),
        P(None, ("dp", "tp"), None, None),
        P("dp"),
        P("section", "dp"),
        P("section", None),
        P("section", None),
        P("section", None, "tp"),
        P("section", None, "tp"),
        P("section", None, "tp"),
        P("section", "tp", None),
    )
    out_specs = (P("section", ("dp", "tp"), None, None), P("section", ("dp", "tp"), None, None))
    return jax.shard_map(shards, mesh=mesh, in_specs=in_specs, out_specs=out_specs, check_vma=False)
```

```python
import functools

import jax
import jax.numpy as jnp
import numpy as np
from jax import lax
from jax.experimental import pallas as pl
from jax.experimental.pallas import tpu as pltpu
from jax.sharding import PartitionSpec as P

HEAD_WIDTH = 128
EPSILON = 1e-06
SOFT_CAP = 50.0
QUERY_SCALE = 144.0 ** (-0.5)

VMEM = pl.BlockSpec(memory_space=pltpu.VMEM)
SMEM = pl.BlockSpec(memory_space=pltpu.SMEM)
HBM = pl.BlockSpec(memory_space=pltpu.HBM)
F32 = jnp.float32
BF16 = jnp.bfloat16


N_HELD = 9


def vmem_out(shape, dtype=BF16):
    return pltpu.VMEM(shape, dtype)


def chunks_of(seq_len):
    half, quarter = seq_len // 2, seq_len // 4
    return tuple(
        (c, c + half, tuple((p, p + quarter) for p in range(c, c + half, quarter)))
        for c in range(0, seq_len, half)
    )


def rotary_tables(seq_len):
    half = HEAD_WIDTH // 2
    freq = np.float32(10000.0) ** (np.float32(-2.0) * np.arange(half, dtype=np.float32) / np.float32(HEAD_WIDTH))
    angle = np.arange(seq_len, dtype=np.float32)[:, None] * freq[None, :]
    cosine, sine = np.cos(angle), np.sin(angle)
    return (
        np.concatenate([cosine, cosine], 1).astype(np.float32),
        np.concatenate([-sine, sine], 1).astype(np.float32),
    )


def rotate(values, cosine, sine):
    return values * cosine + pltpu.roll(values, HEAD_WIDTH // 2, 1) * sine


def column_steps(width):
    step = next(s for s in (768, 512, 384, 256, 128, width) if width % s == 0)
    return [(c, step) for c in range(0, width, step)]


def attend(normed, first, length, cosine, sine, prev, wq, wk, wv, wo, ready, sinks, kv_sinks):
    rows = normed.shape[0]
    kv_cols = wk.shape[1]
    group = wq.shape[1] // kv_cols
    total = first + rows
    heads = [slice(c, c + HEAD_WIDTH) for c in range(0, kv_cols, HEAD_WIDTH)]
    dot = functools.partial(jnp.dot, preferred_element_type=F32)

    def padded(values):
        if rows >= 128:
            return values
        return jnp.concatenate([values, jnp.zeros((128 - rows, values.shape[1]), values.dtype)], 0)

    full = padded(normed)
    ready("k")
    keys = dot(full, wk[...])[:rows]
    ready("v")
    vals = dot(full, wv[...])[:rows].astype(BF16)
    ready("q")
    queries = dot(full, wq[...])[:rows]
    keys = [rotate(keys[:, h], cosine, sine).astype(BF16) for h in heads]
    if kv_sinks is not None:
        for h, key in zip(heads, keys):
            kv_sinks[0][:, h] = key
        kv_sinks[1][...] = vals
    vals = [vals[:, h] for h in heads]
    if prev is not None:
        keys = [jnp.concatenate([prev[0][:, h], key], 0) for h, key in zip(heads, keys)]
        vals = [jnp.concatenate([prev[1][:, h], val], 0) for h, val in zip(heads, vals)]
    vals = [jnp.concatenate([val, jnp.ones_like(val)], 1) for val in vals]
    stacked = []
    for g in range(len(heads)):
        parts = [slice(c, c + HEAD_WIDTH) for c in range(g * group * HEAD_WIDTH, (g + 1) * group * HEAD_WIDTH, HEAD_WIDTH)]
        stacked.append(jnp.concatenate([rotate(queries[:, p], cosine, sine) for p in parts], 0).astype(BF16))
    q_pos = lax.broadcasted_iota(jnp.int32, (rows, total), 0) + first
    k_pos = lax.broadcasted_iota(jnp.int32, (rows, total), 1)
    allowed = (k_pos <= q_pos) & (k_pos < length)
    allowed = jnp.concatenate([allowed] * group, 0)
    scores = [
        lax.dot_general(q, k, (((1,), (1,)), ((), ())), preferred_element_type=F32)
        for q, k in zip(stacked, keys)
    ]
    raised = [
        jnp.where(allowed, jnp.exp(SOFT_CAP * jnp.tanh(s * (QUERY_SCALE / SOFT_CAP))), 0.0).astype(BF16)
        for s in scores
    ]
    outs = [dot(r, v) for r, v in zip(raised, vals)]
    outs = [(o[:, :HEAD_WIDTH] / o[:, HEAD_WIDTH:]).astype(BF16) for o in outs]
    mixed = jnp.concatenate([o[j * rows : (j + 1) * rows] for o in outs for j in range(group)], 1)
    mixed = padded(mixed)
    ready("o")
    for c, step in column_steps(wo.shape[1]):
        part = dot(mixed, wo[:, c : c + step])[:rows].astype(BF16)
        for (a, b), sink in sinks:
            sink[:, c : c + step] = part[a - first : b - first]


def length_of(lengths, sequence):
    at = lax.broadcasted_iota(jnp.int32, lengths.shape, 1) == sequence
    return jnp.sum(jnp.where(at, lengths[...], 0), -1, keepdims=True)


def normalize(values, gain):
    return values * lax.rsqrt(jnp.mean(values * values, -1, keepdims=True) + EPSILON) * gain


def own_kernel(axis, spans, nx, *refs):
    xs, refs = refs[:nx], refs[nx:]
    held, refs = refs[:N_HELD], refs[N_HELD:]
    outs, refs = refs[: len(spans)], refs[len(spans) :]
    kept, sems = refs[:N_HELD], refs[N_HELD]
    copies = [pltpu.make_async_copy(s, t, sems.at[i]) for i, (s, t) in enumerate(zip(held, kept))]
    for copy in copies:
        copy.start()
    pre_gain, _, cosine, sine, lengths, wk, wv, wq, wo = kept
    for copy in copies[: N_HELD - 4]:
        copy.wait()
    waits = dict(zip("kvqo", copies[N_HELD - 4 :]))
    normed = jnp.concatenate([normalize(x[...].astype(F32), pre_gain[...]).astype(BF16) for x in xs], 0)
    length = length_of(lengths, lax.axis_index(axis))
    attend(
        normed, 0, length, cosine[...], sine[...], None, wq, wk, wv, wo,
        lambda name: waits[name].wait(), list(zip(spans, outs)), None,
    )


def peer_kernel(axis, distance, first, spans, keep, x, *refs):
    (pre_gain, _, cosine, sine, lengths, wk, wv, wq, wo), refs = refs[:N_HELD], refs[N_HELD:]
    prev = None
    if first:
        prev, refs = refs[:2], refs[2:]
    outs, refs = refs[: len(spans)], refs[len(spans) :]
    n = lengths.shape[1]
    length = length_of(lengths, lax.rem(lax.axis_index(axis) + (n - distance), n))
    normed = normalize(x[...].astype(F32), pre_gain[...]).astype(BF16)
    rows = slice(first, first + x.shape[0])
    attend(
        normed, first, length, cosine[rows, :], sine[rows, :], prev, wq, wk, wv, wo,
        lambda name: None, list(zip(spans, outs)), refs[:2] if keep else None,
    )


def finish_kernel(offset, *refs):
    own, x, gain = refs[:3]
    others, out = refs[3:-1], refs[-1]
    rows = own.shape[0]
    branch = own[...].astype(F32)
    for other in others:
        branch = branch + other[...].astype(F32)
    held = x[offset : offset + rows, :].astype(F32)
    out[...] = (held + normalize(branch, gain[...])).astype(BF16)


def store_kernel(spans, order, fresh_rows, *refs):
    pieces, out, fresh, chosen, sems = refs[: len(spans)], *refs[-4:]
    pick = pltpu.make_async_copy(order, chosen, sems.at[len(spans)])
    pick.start()
    copies = [
        pltpu.make_async_copy(p, out.at[0, 0, a:b], sems.at[i])
        for i, (p, (a, b)) in enumerate(zip(pieces, spans))
    ]
    for c in copies:
        c.start()
    pick.wait()
    enter = pltpu.make_async_copy(fresh_rows.at[chosen[0], 0], fresh, sems.at[len(spans)])
    enter.start()
    for c in copies:
        c.wait()
    enter.wait()


def advance_kernel(axis, spans, *refs):
    pieces, fresh, out, sems = refs[: len(spans)], *refs[-3:]
    first = lax.axis_index(axis) == 0

    @pl.when(first)
    def _():
        copy = pltpu.make_async_copy(fresh, out.at[0, 0], sems.at[0])
        copy.start()
        copy.wait()

    @pl.when(jnp.logical_not(first))
    def _():
        copies = [
            pltpu.make_async_copy(p, out.at[0, 0, a:b], sems.at[i])
            for i, (p, (a, b)) in enumerate(zip(pieces, spans))
        ]
        for c in copies:
            c.start()
        for c in copies:
            c.wait()


def split_kernel(spans, x, *refs):
    outs, sems = refs[:-1], refs[-1]
    copies = [
        pltpu.make_async_copy(x.at[0, 0, a:b], out, sems.at[i])
        for i, (out, (a, b)) in enumerate(zip(outs, spans))
    ]
    for c in copies:
        c.start()
    for c in copies:
        c.wait()


def call(kernel, name, out_shape, in_specs, out_specs, args, scratch=(), us=1.0, limit=16 << 20):
    args = [pltpu.with_memory_space_constraint(a, pltpu.HBM) if s is HBM else a for a, s in zip(args, in_specs)]
    return pl.pallas_call(
        kernel,
        out_shape=out_shape,
        in_specs=in_specs,
        out_specs=out_specs,
        scratch_shapes=list(scratch),
        name=name,
        cost_estimate=pl.CostEstimate(flops=int(us * 1e7), bytes_accessed=1024, transcendentals=0),
        compiler_params=pltpu.CompilerParams(vmem_limit_bytes=limit),
    )(*args)


def shards(
    incoming,
    fresh_rows,
    entry_order,
    flight_lengths,
    pre_gain,
    post_gain,
    w_query,
    key_weight,
    value_weight,
    w_out,
):
    seq_len, model = incoming.shape[2:]
    chunks = chunks_of(seq_len)
    spans = [span for _, _, inner in chunks for span in inner]
    n_tp = lax.axis_size("tp")
    n_section = lax.axis_size("section")
    kv_cols = key_weight.shape[2]
    cosine, sine = (jnp.asarray(t) for t in rotary_tables(seq_len))
    held = [pre_gain, post_gain, cosine, sine, flight_lengths, key_weight[0], value_weight[0], w_query[0], w_out[0]]
    dma = pltpu.SemaphoreType.DMA

    xs = call(
        functools.partial(split_kernel, [(a, b) for a, b, _ in chunks]), "split",
        [vmem_out((b - a, model)) for a, b, _ in chunks], [HBM], [VMEM] * len(chunks),
        [incoming], [dma((len(chunks),))],
    )
    ahead = {d: [(i, (i + d) % n_tp) for i in range(n_tp)] for d in range(1, n_tp)}
    arrived = {d: [lax.ppermute(x, "tp", ahead[d]) for x in xs] for d in ahead}

    own = call(
        functools.partial(own_kernel, "tp", spans, len(xs)), "own",
        [vmem_out((b - a, model)) for a, b in spans] + [vmem_out(h.shape, h.dtype) for h in held],
        [VMEM] * len(xs) + [HBM] * N_HELD, [VMEM] * (len(spans) + N_HELD),
        [*xs, *held], [dma((N_HELD,))], us=6.0,
    )
    own, held = own[: len(spans)], own[len(spans) :]

    back = {span: [] for span in spans}
    for d in ahead:
        kept = []
        for c, (first, last, inner) in enumerate(chunks):
            keep = c + 1 < len(chunks)
            shapes = [vmem_out((b - a, model)) for a, b in inner]
            shapes += [vmem_out((last - first, kv_cols))] * 2 if keep else []
            prev = [jnp.concatenate(k, 0) if len(k) > 1 else k[0] for k in zip(*kept)]
            done = call(
                functools.partial(peer_kernel, "tp", d, first, inner, keep), f"peer{c}",
                shapes, [VMEM] * (1 + N_HELD + len(prev)), [VMEM] * len(shapes),
                [arrived[d][c], *held, *prev], us=3.0,
            )
            kept.append(done[len(inner) :])
            for span, part in zip(inner, done):
                back[span].append(lax.ppermute(part, "tp", [(t, s) for s, t in ahead[d]]))

    produced, moved = [], []
    ring = [(i, (i + 1) % n_section) for i in range(n_section)]
    for c, (first, last, inner) in enumerate(chunks):
        for span in inner:
            piece = call(
                functools.partial(finish_kernel, span[0] - first), "finish",
                vmem_out((span[1] - span[0], model)), [VMEM] * (3 + len(back[span])), VMEM,
                [own[spans.index(span)], xs[c], held[1], *back[span]], us=0.3,
            )
            produced.append(piece)
            moved.append(lax.ppermute(piece, "section", ring))
    full = jax.ShapeDtypeStruct(incoming.shape, incoming.dtype)
    stored, fresh = call(
        functools.partial(store_kernel, spans), "store",
        [full, vmem_out((seq_len, model))], [HBM, HBM] + [VMEM] * len(spans), [HBM, VMEM],
        [entry_order, fresh_rows, *produced],
        [pltpu.SMEM(entry_order.shape, entry_order.dtype), dma((len(spans) + 1,))], us=1.5,
    )
    advanced = call(
        functools.partial(advance_kernel, "section", spans), "advance", full,
        [VMEM] * (len(spans) + 1), HBM, [*moved, fresh], [dma((len(spans),))],
    )
    return stored, advanced


def solution(mesh):
    in_specs = (
        P("section", ("dp", "tp"), None, None),
        P(None, ("dp", "tp"), None, None),
        P("dp"),
        P("section", "dp"),
        P("section", None),
        P("section", None),
        P("section", None, "tp"),
        P("section", None, "tp"),
        P("section", None, "tp"),
        P("section", "tp", None),
    )
    out_specs = (P("section", ("dp", "tp"), None, None), P("section", ("dp", "tp"), None, None))
    return jax.shard_map(shards, mesh=mesh, in_specs=in_specs, out_specs=out_specs, check_vma=False)
```
